32 devices in a mesh: lat: 4 (over z), lon: 8 (over y, x, core).
Axes of the slice: x: 2, y: 2, z: 4, core: 2. Of those that a mesh axis runs over, the one named last changes fastest.
Arguments:
- inputs: bfloat16 [4, 32, 256, 800], P(None, 'lat', 'lon'), may hold values from -6 to 6
- conv_kernel: bfloat16 [7, 7, 800], replicated, may hold values from -0.875 to 0.875
- norm_gain: bfloat16 [800], replicated, may hold values from 0.5 to 1.5
- norm_shift: bfloat16 [800], replicated, may hold values from -3 to 3
- w_in: bfloat16 [800, 3200], replicated, may hold values from -0.21875 to 0.21875
- b_in: bfloat16 [3200], replicated, may hold values from -3 to 3
- w_out: bfloat16 [3200, 800], replicated, may hold values from -0.109375 to 0.109375
- b_out: bfloat16 [800], replicated, may hold values from -3 to 3
- ocean_mask: int32 [32, 256], P('lat', 'lon'), may hold values from 0 to 1, as said below
- lengths: int32 [4], replicated, may hold values from 1 to 8, as said below
- cotangent: bfloat16 [4, 32, 256, 800], P(None, 'lat', 'lon'), may hold values from -6 to 6
Outputs:
- output: bfloat16 [4, 32, 256, 800], P(None, 'lat', 'lon')
- d_inputs: bfloat16 [4, 32, 256, 800], P(None, 'lat', 'lon')
- d_kernel: float32 [7, 7, 800], replicated
- d_gain: float32 [800], replicated
- d_shift: float32 [800], replicated
- d_w_in: float32 [800, 3200], replicated
- d_b_in: float32 [3200], replicated
- d_w_out: float32 [3200, 800], replicated
- d_b_out: float32 [800], replicated
The draws below stay inside these ranges and needn't reach their ends.
Inputs may be any that keep to these rules, and one draw needn't show every extreme that they name: `ocean_mask`: a 0/1 mask; the last latitude row is all ocean. `lengths`: some micro-batch completes the whole rollout.
All inputs are finite; a program needn't handle non-finite values.
Results may differ from the reference program's by a relative error of at most 0.0063.
Values may be sent and summed in bfloat16 or wider, within the bound.
A program may use at most 128 MiB of HBM per device.

```python
import jax
import jax.numpy as jnp
from jax import lax

C = 800
HID = 3200
KS = 7
ROLLOUT = 8
MB = 4
H = 32
W = 256


def draw_ocean_mask(key, part):
    lat_index = lax.broadcasted_iota(jnp.int32, (H, W), 0)
    lon_index = lax.broadcasted_iota(jnp.int32, (H, W), 1)
    threshold = 150 + 350 * lat_index // H + 350 * lon_index // W
    draws = jax.random.randint(key, (H, W), 0, 1000)
    ocean = (draws < threshold).astype(jnp.int32)
    return jnp.where(lat_index == H - 1, 1, ocean).astype(jnp.int32)


def draw_lengths(key, part):
    steps_done = jax.random.randint(jax.random.fold_in(key, 1), (MB,), 1, ROLLOUT + 1)
    full_one = jax.random.randint(jax.random.fold_in(key, 2), (), 0, MB)
    position = lax.iota(jnp.int32, MB)
    return jnp.where(position == full_one, ROLLOUT, steps_done).astype(jnp.int32)


def block_scale(key, shape, pieces, least, top_value):
    gain, own = 1.0, jax.random.fold_in(key, 6)
    for axis_at, shards_of in pieces:
        heights = jnp.exp(jax.random.uniform(jax.random.fold_in(own, axis_at), (shards_of,), jnp.float32, least / len(pieces), top_value / len(pieces)))
        gain = gain * jnp.repeat(heights, shape[axis_at] // shards_of).reshape([-1 if axis == axis_at else 1 for axis in range(len(shape))])
    return gain


def noise(key, dims, spread, most, split=(), kind=jnp.bfloat16):
    loudness = block_scale(key, dims, split, -0.22, 0.18) if split else 1.0
    values = jax.random.normal(key, dims, jnp.float32) * spread * loudness
    return jnp.minimum(jnp.maximum(values, -most), most).astype(kind)


def setup_inputs(seed: int = 0) -> dict:
    seeds = jax.random.split(jax.random.key(seed), 12)
    return {
        "inputs": noise(seeds[0], (MB, H, W, C), 1.0, 6.0, ((1, 4), (2, 8))),
        "conv_kernel": noise(seeds[1], (KS, KS, C), (KS * KS) ** -0.5, 0.875),
        "norm_gain": jnp.clip(1.0 + 0.1 * jax.random.normal(seeds[2], (C,), jnp.float32), 0.5, 1.5).astype(jnp.bfloat16),
        "norm_shift": noise(seeds[3], (C,), 0.5, 3.0),
        "w_in": noise(seeds[4], (C, HID), C ** -0.5, 0.21875),
        "b_in": noise(seeds[5], (HID,), 0.5, 3.0),
        "w_out": noise(seeds[6], (HID, C), HID ** -0.5, 0.109375),
        "b_out": noise(seeds[7], (C,), 0.5, 3.0),
        "ocean_mask": draw_ocean_mask(jax.random.fold_in(seeds[11], 71), 0),
        "lengths": draw_lengths(jax.random.fold_in(seeds[11], 71), 0),
        "cotangent": noise(seeds[10], (MB, H, W, C), 1.0, 6.0, ((1, 4), (2, 8))),
    }


epsilon = 1e-05

@jax.custom_vjp
def low(v):
    return lax.optimization_barrier(v.astype(jnp.bfloat16)).astype(jnp.float32)

@jax.custom_vjp
def low_back(v):
    return v

def low_keep(v):
    return (low(v), None)

def low_pass(kept, grad):
    return (grad,)

def back_keep(v):
    return (v, None)

def back_low(kept, grad):
    return (low(grad),)
low.defvjp(low_keep, low_pass)
low_back.defvjp(back_keep, back_low)

def reference(inputs, conv_kernel, norm_gain, norm_shift, w_in, b_in, w_out, b_out, ocean_mask, lengths, cotangent):
    highest = lax.Precision.HIGHEST
    half_side = KS // 2
    ocean_cells = ocean_mask.astype(jnp.float32)[None, :, :, None]
    cell_count = jnp.sum(ocean_mask).astype(jnp.float32) * inputs.shape[0]
    channels = inputs.shape[3]

    def forward(source, kernel, gain_vec, shift_vec, weight_in, bias_in, weight_out, bias_out):
        padded = jnp.pad(source, ((0, 0), (half_side, half_side), (half_side, half_side), (0, 0)))
        convolved = jnp.zeros(source.shape, jnp.float32)
        for row_shift in range(KS):
            for col_shift in range(KS):
                convolved = convolved + kernel[row_shift, col_shift] * padded[:, row_shift:row_shift + source.shape[1], col_shift:col_shift + source.shape[2]]
        convolved = low_back(convolved)
        mean_value = lax.optimization_barrier(jnp.sum(convolved * ocean_cells, axis=(0, 1, 2))) / cell_count
        centered = convolved - mean_value
        variance = lax.optimization_barrier(jnp.sum(centered * centered * ocean_cells, axis=(0, 1, 2))) / cell_count
        standard = centered * lax.rsqrt(variance + epsilon)
        normed = low(standard * gain_vec + shift_vec).reshape(-1, channels)
        first_mm = low_back(jnp.dot(normed, weight_in, precision=highest))
        activated = low(jax.nn.gelu(first_mm + bias_in, approximate=True))
        second_mm = low_back(jnp.dot(activated, weight_out, precision=highest))
        branch = (second_mm + bias_out).reshape(source.shape)
        return source + ocean_cells * branch
    primals = [a.astype(jnp.float32) for a in (inputs, conv_kernel, norm_gain, norm_shift, w_in, b_in, w_out, b_out)]
    result, pullback = jax.vjp(forward, *primals)
    kept_steps = lengths.astype(jnp.float32) / ROLLOUT
    d_result = cotangent.astype(jnp.float32) * kept_steps[:, None, None, None]
    grads = pullback(d_result)
    return (result.astype(jnp.bfloat16), grads[0].astype(jnp.bfloat16), grads[1], grads[2], grads[3], grads[4], grads[5], grads[6], grads[7])
```

```python
import functools

import jax
import jax.numpy as jnp
from jax import lax
from jax.experimental import pallas as pl
from jax.experimental.pallas import tpu as pltpu
from jax.sharding import PartitionSpec as P

KS = 7
ROLLOUT = 8
HALF = KS // 2
EDGE = 8
epsilon = 1e-05
F32 = jnp.float32
BF16 = jnp.bfloat16
MESH = pl.DeviceIdType.MESH


def with_halo(value):
    for axis, dim, width in (("lat", 1, HALF), ("lon", 2, EDGE)):
        count, length = (lax.axis_size(axis), value.shape[dim])
        up = [(i, (i + 1) % count) for i in range(count - 1)]
        down = [(j, i) for i, j in up]
        last = lax.slice_in_dim(value, length - width, length, axis=dim)
        initial = lax.slice_in_dim(value, 0, width, axis=dim)
        before = lax.ppermute(last, axis, up)
        after = lax.ppermute(initial, axis, down)
        value = jnp.concatenate([before, value, after], axis=dim)
    return value


def merge_sum(slots, count):
    total = slots[0]
    for k in range(1, count):
        total = total + slots[k]
    return total


def merge_moments(slots, count):
    cells = slots[0][2:3]
    weighted = slots[0][2:3] * slots[0][0:1]
    for k in range(1, count):
        cells = cells + slots[k][2:3]
        weighted = weighted + slots[k][2:3] * slots[k][0:1]
    mean = weighted / jnp.maximum(cells, 1.0)
    squares = None
    for k in range(count):
        off = slots[k][0:1] - mean
        term = slots[k][1:2] + slots[k][2:3] * off * off
        squares = term if squares is None else squares + term
    return jnp.concatenate([mean, squares, cells, jnp.zeros((5, mean.shape[1]), F32)], axis=0)


def exchange_kernel(merge, sizes, x_ref, o_ref, buf0, mid, buf1, send0, recv0, send1, recv1):
    axes = ("lat", "lon")
    barrier = pltpu.get_barrier_semaphore()
    places = [lax.axis_index(a) for a in axes]
    for axis, size, me in zip(axes, sizes, places):
        for d in range(1, size):
            pl.semaphore_signal(
                barrier, inc=1, device_id={axis: lax.rem(me + d, size)}, device_id_type=MESH
            )
    pl.semaphore_wait(barrier, sum(sizes) - 2)
    stages = ((x_ref, buf0, send0, recv0, mid), (mid, buf1, send1, recv1, o_ref))
    for axis, size, me, (src, buf, send, recv, dst) in zip(axes, sizes, places, stages):
        copies = []
        for d in range(1, size):
            copy = pltpu.make_async_remote_copy(
                src_ref=src,
                dst_ref=buf.at[me],
                send_sem=send.at[d],
                recv_sem=recv.at[me],
                device_id={axis: lax.rem(me + d, size)},
                device_id_type=MESH,
            )
            copy.start()
            copies.append(copy)
        buf[me] = src[...]
        for d in range(1, size):
            other = lax.rem(me + d, size)
            pltpu.make_async_remote_copy(
                src_ref=src,
                dst_ref=buf.at[other],
                send_sem=send.at[d],
                recv_sem=recv.at[other],
                device_id={axis: other},
                device_id_type=MESH,
            ).wait_recv()
        dst[...] = merge([buf[k] for k in range(size)], size)
        for copy in copies:
            copy.wait_send()


def exchange(merge, value, number):
    sizes = (lax.axis_size("lat"), lax.axis_size("lon"))
    rows, lanes = value.shape
    return pl.pallas_call(
        functools.partial(exchange_kernel, merge, sizes),
        out_shape=jax.ShapeDtypeStruct(value.shape, F32),
        in_specs=[pl.BlockSpec(memory_space=pltpu.VMEM)],
        out_specs=pl.BlockSpec(memory_space=pltpu.VMEM),
        scratch_shapes=[
            pltpu.VMEM((sizes[0], rows, lanes), F32),
            pltpu.VMEM((rows, lanes), F32),
            pltpu.VMEM((sizes[1], rows, lanes), F32),
            pltpu.SemaphoreType.DMA((sizes[0],)),
            pltpu.SemaphoreType.DMA((sizes[0],)),
            pltpu.SemaphoreType.DMA((sizes[1],)),
            pltpu.SemaphoreType.DMA((sizes[1],)),
        ],
        compiler_params=pltpu.CompilerParams(collective_id=number, has_side_effects=True),
        name="exchange" + str(number),
    )(value)


def spread_kernel(ker_ref, taps):
    for t in range(KS * KS):
        taps[t] = jnp.broadcast_to(ker_ref[t : t + 1, :].astype(F32), (8, 128))


def conv_tile(rows_ref, taps, strip, height, flip):
    sums = [None] * height
    for j in range(KS):
        column = [taps[KS * KS - 1 - (i * KS + j) if flip else i * KS + j] for i in range(KS)]
        for r in range(height + KS - 1):
            x = rows_ref[r, pl.ds(strip * 8 + EDGE - HALF + j, 8), :]
            for i in range(KS):
                h = r - i
                if 0 <= h < height:
                    term = column[i] * x
                    sums[h] = term if sums[h] is None else sums[h] + term
    return sums


def forward_kernel(p_ref, ker_ref, o_ref, rows_ref, taps):
    batches, height, width, _ = o_ref.shape
    spread_kernel(ker_ref, taps)

    def batch(m, carry):
        for r in range(height + KS - 1):
            rows_ref[r] = p_ref[m, r].astype(F32)
        for strip in range(width // 8):
            sums = conv_tile(rows_ref, taps, strip, height, False)
            for h in range(height):
                o_ref[m, h, pl.ds(strip * 8, 8), :] = sums[h]
        return carry

    lax.fori_loop(0, batches, batch, 0)


def depthwise(padded, kernel, shape):
    batches, height, width, channels = shape
    tall, wide = height + KS - 1, width + 2 * EDGE
    return pl.pallas_call(
        forward_kernel,
        grid=(pl.cdiv(channels, 128),),
        in_specs=[
            pl.BlockSpec((batches, tall, wide, 128), lambda c: (0, 0, 0, c)),
            pl.BlockSpec((KS * KS, 128), lambda c: (0, c)),
        ],
        out_specs=pl.BlockSpec((batches, height, width, 128), lambda c: (0, 0, 0, c)),
        out_shape=jax.ShapeDtypeStruct(shape, F32),
        scratch_shapes=[pltpu.VMEM((tall, wide, 128), F32), pltpu.VMEM((KS * KS, 8, 128), F32)],
        name="depthwise",
    )(padded, kernel)


def backward_kernel(
    p_ref, d_ref, ker_ref, g_ref, share_ref, o_ref, k_ref, rows_ref, grads_ref, taps, sums_ref
):
    batches, height, width, _ = o_ref.shape
    spread_kernel(ker_ref, taps)
    sums_ref[...] = jnp.zeros_like(sums_ref)

    def batch(m, carry):
        for r in range(height + KS - 1):
            rows_ref[r] = p_ref[m, r].astype(F32)
            grads_ref[r] = d_ref[m, r].astype(F32)
        share = share_ref[m]
        for strip in range(width // 8):
            sums = conv_tile(grads_ref, taps, strip, height, True)
            for h in range(height):
                g = g_ref[m, h, pl.ds(strip * 8, 8), :].astype(F32) * share
                o_ref[m, h, pl.ds(strip * 8, 8), :] = (g + sums[h]).astype(BF16)
            own = [grads_ref[h + HALF, pl.ds(strip * 8 + EDGE, 8), :] for h in range(height)]
            for j in range(KS):
                parts = [sums_ref[i * KS + j] for i in range(KS)]
                for r in range(height + KS - 1):
                    x = rows_ref[r, pl.ds(strip * 8 + EDGE - HALF + j, 8), :]
                    for i in range(KS):
                        h = r - i
                        if 0 <= h < height:
                            parts[i] = parts[i] + own[h] * x
                for i in range(KS):
                    sums_ref[i * KS + j] = parts[i]
        return carry

    lax.fori_loop(0, batches, batch, 0)
    for t in range(KS * KS):
        k_ref[t : t + 1, :] = jnp.sum(sums_ref[t], axis=0, keepdims=True)


def depthwise_back(padded, d_padded, kernel, cotangent, shares):
    batches, height, width, channels = cotangent.shape
    tall, wide = height + KS - 1, width + 2 * EDGE
    tile = pl.BlockSpec((batches, tall, wide, 128), lambda c: (0, 0, 0, c))
    own = pl.BlockSpec((batches, height, width, 128), lambda c: (0, 0, 0, c))
    taps = pl.BlockSpec((KS * KS, 128), lambda c: (0, c))
    return pl.pallas_call(
        backward_kernel,
        grid=(pl.cdiv(channels, 128),),
        in_specs=[tile, tile, taps, own, pl.BlockSpec(memory_space=pltpu.SMEM)],
        out_specs=[own, taps],
        out_shape=[
            jax.ShapeDtypeStruct(cotangent.shape, BF16),
            jax.ShapeDtypeStruct((KS * KS, channels), F32),
        ],
        scratch_shapes=[
            pltpu.VMEM((tall, wide, 128), F32),
            pltpu.VMEM((tall, wide, 128), F32),
            pltpu.VMEM((KS * KS, 8, 128), F32),
            pltpu.VMEM((KS * KS, 8, 128), F32),
        ],
        name="depthwise_back",
    )(padded, d_padded, kernel, cotangent, shares)


def smooth_gate(values):
    return jax.nn.gelu(values, approximate=True)


def body(
    inputs,
    conv_kernel,
    norm_gain,
    norm_shift,
    w_in,
    b_in,
    w_out,
    b_out,
    ocean_mask,
    lengths,
    cotangent,
):
    batches, tile_rows, tile_cols, channels = inputs.shape
    padded = with_halo(inputs)
    taps = conv_kernel.reshape(KS * KS, channels)
    convolved = depthwise(padded, taps, inputs.shape)
    ocean_cells = ocean_mask.astype(F32)[None, :, :, None]
    local_count = jnp.sum(ocean_mask).astype(F32) * batches
    local_mean = jnp.sum(convolved * ocean_cells, axis=(0, 1, 2)) / jnp.maximum(local_count, 1.0)
    off = convolved - local_mean
    local_squares = jnp.sum(off * off * ocean_cells, axis=(0, 1, 2))
    moments = jnp.zeros((8, channels), F32)
    moments = moments.at[0].set(local_mean).at[1].set(local_squares).at[2].set(local_count)
    moments = exchange(merge_moments, moments, 0)
    mean_value, cell_count = moments[0], moments[2, 0]
    inv_std = lax.rsqrt(moments[1] / cell_count + epsilon)
    standard = (convolved - mean_value) * inv_std
    gain_vec = norm_gain.astype(F32)
    normed = (standard * gain_vec + norm_shift.astype(F32)).astype(BF16).reshape(-1, channels)
    pre_gate = jnp.dot(normed, w_in, preferred_element_type=F32) + b_in.astype(F32)
    activated, gate_back = jax.vjp(smooth_gate, pre_gate)
    act_low = activated.astype(BF16)
    branch = jnp.dot(act_low, w_out, preferred_element_type=F32) + b_out.astype(F32)
    output = (inputs.astype(F32) + ocean_cells * branch.reshape(inputs.shape)).astype(BF16)
    kept_steps = lengths.astype(F32) / ROLLOUT
    d_output = cotangent.astype(F32) * kept_steps[:, None, None, None]
    d_branch = (d_output * ocean_cells).reshape(-1, channels)
    branch_low = d_branch.astype(BF16)
    local_b_out = jnp.sum(d_branch, axis=0)
    local_w_out = lax.dot_general(
        act_low, branch_low, (((0,), (0,)), ((), ())), preferred_element_type=F32
    ).astype(BF16)
    d_act = lax.dot_general(branch_low, w_out, (((1,), (1,)), ((), ())), preferred_element_type=F32)
    d_pre = gate_back(d_act)[0]
    pre_low = d_pre.astype(BF16)
    local_b_in = jnp.sum(d_pre, axis=0)
    local_w_in = lax.dot_general(
        normed, pre_low, (((0,), (0,)), ((), ())), preferred_element_type=F32
    ).astype(BF16)
    d_normed = lax.dot_general(
        pre_low, w_in, (((1,), (1,)), ((), ())), preferred_element_type=F32
    ).reshape(inputs.shape)
    sums = jnp.zeros((8, channels), F32)
    sums = sums.at[0].set(jnp.sum(d_normed, axis=(0, 1, 2)))
    sums = sums.at[1].set(jnp.sum(d_normed * standard, axis=(0, 1, 2)))
    sums = sums.at[2].set(local_b_out)
    spread = pl.cdiv(b_in.shape[0], channels)
    sums = sums.at[3 : 3 + spread].set(
        jnp.pad(local_b_in, (0, spread * channels - b_in.shape[0])).reshape(spread, channels)
    )
    sums = exchange(merge_sum, sums, 1)
    d_shift, d_gain, d_b_out = sums[0], sums[1], sums[2]
    d_b_in = sums[3 : 3 + spread].reshape(-1)[: b_in.shape[0]]
    d_conv = (
        gain_vec * inv_std * (d_normed - ocean_cells * (d_shift + standard * d_gain) / cell_count)
    )
    d_padded = with_halo(d_conv.astype(BF16))
    d_inputs, local_kernel = depthwise_back(padded, d_padded, taps, cotangent, kept_steps)
    d_w_in, d_w_out = lax.psum((local_w_in, local_w_out), ("lat", "lon"))
    d_kernel = lax.psum(local_kernel, ("lat", "lon"))
    return (
        output,
        d_inputs,
        d_kernel.reshape(conv_kernel.shape),
        d_gain,
        d_shift,
        d_w_in.astype(F32),
        d_b_in,
        d_w_out.astype(F32),
        d_b_out,
    )


def solution(mesh):
    tile = P(None, "lat", "lon", None)
    in_specs = (tile, P(), P(), P(), P(), P(), P(), P(), P("lat", "lon"), P(), tile)
    out_specs = (tile, tile, P(), P(), P(), P(), P(), P(), P())
    return jax.shard_map(body, mesh=mesh, in_specs=in_specs, out_specs=out_specs, check_vma=False)
```

```python
import functools

import jax
import jax.numpy as jnp
from jax import lax
from jax.experimental import pallas as pl
from jax.experimental.pallas import tpu as pltpu
from jax.sharding import PartitionSpec as P

KS = 7
ROLLOUT = 8
HALF = KS // 2
EDGE = 8
UNITS = 16
LAG = 2
epsilon = 1e-05
F32 = jnp.float32
BF16 = jnp.bfloat16
MESH = pl.DeviceIdType.MESH


def with_halo(value):
    for axis, dim, width in (("lat", 1, HALF), ("lon", 2, EDGE)):
        count, length = (lax.axis_size(axis), value.shape[dim])
        up = [(i, (i + 1) % count) for i in range(count - 1)]
        down = [(j, i) for i, j in up]
        last = lax.slice_in_dim(value, length - width, length, axis=dim)
        initial = lax.slice_in_dim(value, 0, width, axis=dim)
        before = lax.ppermute(last, axis, up)
        after = lax.ppermute(initial, axis, down)
        value = jnp.concatenate([before, value, after], axis=dim)
    return value


def merge_sum(slots, count):
    total = slots[0]
    for k in range(1, count):
        total = total + slots[k]
    return total


def merge_moments(slots, count):
    cells = slots[0][2:3]
    weighted = slots[0][2:3] * slots[0][0:1]
    for k in range(1, count):
        cells = cells + slots[k][2:3]
        weighted = weighted + slots[k][2:3] * slots[k][0:1]
    mean = weighted / jnp.maximum(cells, 1.0)
    squares = None
    for k in range(count):
        off = slots[k][0:1] - mean
        term = slots[k][1:2] + slots[k][2:3] * off * off
        squares = term if squares is None else squares + term
    return jnp.concatenate([mean, squares, cells, jnp.zeros((5, mean.shape[1]), F32)], axis=0)


def exchange_kernel(merge, sizes, x_ref, o_ref, buf0, mid, buf1, send0, recv0, send1, recv1):
    axes = ("lat", "lon")
    barrier = pltpu.get_barrier_semaphore()
    places = [lax.axis_index(a) for a in axes]
    for axis, size, me in zip(axes, sizes, places):
        for d in range(1, size):
            pl.semaphore_signal(
                barrier, inc=1, device_id={axis: lax.rem(me + d, size)}, device_id_type=MESH
            )
    pl.semaphore_wait(barrier, sum(sizes) - 2)
    stages = ((x_ref, buf0, send0, recv0, mid), (mid, buf1, send1, recv1, o_ref))
    for axis, size, me, (src, buf, send, recv, dst) in zip(axes, sizes, places, stages):
        copies = []
        for d in range(1, size):
            copy = pltpu.make_async_remote_copy(
                src_ref=src,
                dst_ref=buf.at[me],
                send_sem=send.at[d],
                recv_sem=recv.at[me],
                device_id={axis: lax.rem(me + d, size)},
                device_id_type=MESH,
            )
            copy.start()
            copies.append(copy)
        buf[me] = src[...]
        for d in range(1, size):
            other = lax.rem(me + d, size)
            pltpu.make_async_remote_copy(
                src_ref=src,
                dst_ref=buf.at[other],
                send_sem=send.at[d],
                recv_sem=recv.at[other],
                device_id={axis: other},
                device_id_type=MESH,
            ).wait_recv()
        dst[...] = merge([buf[k] for k in range(size)], size)
        for copy in copies:
            copy.wait_send()


def exchange(merge, value, number):
    sizes = (lax.axis_size("lat"), lax.axis_size("lon"))
    rows, lanes = value.shape
    return pl.pallas_call(
        functools.partial(exchange_kernel, merge, sizes),
        out_shape=jax.ShapeDtypeStruct(value.shape, F32),
        in_specs=[pl.BlockSpec(memory_space=pltpu.VMEM)],
        out_specs=pl.BlockSpec(memory_space=pltpu.VMEM),
        scratch_shapes=[
            pltpu.VMEM((sizes[0], rows, lanes), F32),
            pltpu.VMEM((rows, lanes), F32),
            pltpu.VMEM((sizes[1], rows, lanes), F32),
            pltpu.SemaphoreType.DMA((sizes[0],)),
            pltpu.SemaphoreType.DMA((sizes[0],)),
            pltpu.SemaphoreType.DMA((sizes[1],)),
            pltpu.SemaphoreType.DMA((sizes[1],)),
        ],
        compiler_params=pltpu.CompilerParams(collective_id=number, has_side_effects=True),
        name="exchange" + str(number),
    )(value)


class Ring:
    STEPS = 9

    def __init__(self, side, lats, grads, result, part, work, land0, land, gat, send, recv, local):
        self.grads, self.result, self.local = grads, result, local
        self.side, self.lats = side, lats
        self.part, self.work, self.land0, self.land, self.gat = part, work, land0, land, gat
        self.send, self.recv = send, recv
        self.units = part.shape[2]
        lon, lat = lax.axis_index("lon"), lax.axis_index("lat")
        core = lax.rem(lon, 2)
        pair = lon // 2
        a, b = pair // side, lax.rem(pair, side)
        first = a * (1 - core) + b * core
        second = b * (1 - core) + a * core
        wide = 2 * side * (1 - core) + 2 * core
        narrow = 2 * (1 - core) + 2 * side * core
        self.core, self.lon = core, lon
        self.axes = (
            (side, first, lambda q: {"lon": lon + (q - first) * wide}),
            (side, second, lambda q: {"lon": lon + (q - second) * narrow}),
            (lats, lat, lambda q: {"lat": q}),
        )
        sub0 = self.units // side
        sub1 = sub0 // side
        sub2 = sub1 // lats
        start0 = first * sub0
        start1 = start0 + second * sub1
        start2 = start1 + lat * sub2
        self.ranges = ((0, start0, sub0), (start0, start1, sub1), (start1, start2, sub2))

    def barrier(self):
        bar = pltpu.get_barrier_semaphore()
        pl.semaphore_signal(
            bar, inc=1, device_id={"lon": self.lon + 1 - 2 * self.core}, device_id_type=MESH
        )
        count = 1
        for size, place, where in self.axes:
            for d in range(1, size):
                pl.semaphore_signal(bar, inc=1, device_id=where(lax.rem(place + d, size)), device_id_type=MESH)
                count += 1
        pl.semaphore_wait(bar, count)

    def load(self, half, c):
        return pltpu.make_async_copy(
            self.grads.at[half, c], self.part.at[half, c], self.local.at[0, half, c]
        )

    def save(self, half, c):
        return pltpu.make_async_copy(
            self.gat.at[half, c], self.result.at[half, c], self.local.at[1, half, c]
        )

    def cores(self, c, out):
        other = 1 - self.core
        src, dst, stage = (
            (self.gat.at[self.core, c], self.gat.at[self.core, c], 7)
            if out
            else (self.part.at[other, c], self.land0.at[c], 0)
        )
        return pltpu.make_async_remote_copy(
            src_ref=src, dst_ref=dst, send_sem=self.send.at[c, stage, 0], recv_sem=self.recv.at[c, stage, 0],
            device_id={"lon": self.lon + 1 - 2 * self.core}, device_id_type=MESH,
        )

    def scatter(self, c, k):
        size, place, where = self.axes[k]
        base, start, sub = self.ranges[k]
        out = []
        for d in range(1, size):
            q = lax.rem(place + d, size)
            out.append(pltpu.make_async_remote_copy(
                src_ref=self.work.at[c, pl.ds(base + q * sub, sub)],
                dst_ref=self.land[k].at[c, d - 1],
                send_sem=self.send.at[c, 1 + k, d - 1], recv_sem=self.recv.at[c, 1 + k, d - 1],
                device_id=where(q), device_id_type=MESH,
            ))
        return out

    def gather(self, c, k):
        size, place, where = self.axes[k]
        base, start, sub = self.ranges[k]
        out = []
        for d in range(1, size):
            q = lax.rem(place + d, size)
            out.append(pltpu.make_async_remote_copy(
                src_ref=self.gat.at[self.core, c, pl.ds(start, sub)],
                dst_ref=self.gat.at[self.core, c, pl.ds(start, sub)],
                send_sem=self.send.at[c, 4 + k, d - 1], recv_sem=self.recv.at[c, 4 + k, d - 1],
                device_id=where(q), device_id_type=MESH,
            ))
        return out

    def add(self, c, k):
        base, start, sub = self.ranges[k]
        total = self.work[c, pl.ds(start, sub)].astype(F32)
        for d in range(self.axes[k][0] - 1):
            total = total + self.land[k][c, d].astype(F32)
        return total.astype(BF16)

    def step(self, s, c):
        if s == 0:
            for half in range(2):
                self.load(half, c).wait()
            self.cores(c, False).start()
        elif s == 1:
            self.cores(c, False).wait()
            self.work[c] = (self.part[self.core, c].astype(F32) + self.land0[c].astype(F32)).astype(BF16)
            for x in self.scatter(c, 0): x.start()
        elif s in (2, 3, 4):
            k = s - 2
            for x in self.scatter(c, k): x.wait()
            base, start, sub = self.ranges[k]
            if k < 2:
                self.work[c, pl.ds(start, sub)] = self.add(c, k)
                for x in self.scatter(c, k + 1): x.start()
            else:
                self.gat[self.core, c, pl.ds(start, sub)] = self.add(c, k)
                for x in self.gather(c, 2): x.start()
        elif s in (5, 6, 7):
            k = 7 - s
            for x in self.gather(c, k): x.wait()
            if k:
                for x in self.gather(c, k - 1): x.start()
            else:
                self.cores(c, True).start()
        else:
            self.cores(c, True).wait()
            for half in range(2):
                self.save(half, c).start()


def reduce_kernel(
    side, lats, grads, result, part, gat, work, land0, land1, land2, land3, send, recv, local
):
    ring = Ring(
        side, lats, grads, result, part, work, land0, (land1, land2, land3), gat, send, recv, local
    )
    chunks = part.shape[1]

    def fetch(c, carry):
        for half in range(2):
            ring.load(half, c).start()
        return carry

    lax.fori_loop(0, chunks, fetch, 0)
    ring.barrier()

    def tick(t, carry):
        for s in reversed(range(Ring.STEPS)):
            c = t - LAG * s

            @pl.when((c >= 0) & (c < chunks))
            def _():
                ring.step(s, c)

        return carry

    lax.fori_loop(0, chunks + LAG * (Ring.STEPS - 1), tick, 0)

    def drain(c, carry):
        for half in range(2):
            ring.save(half, c).wait()
        return carry

    lax.fori_loop(0, chunks, drain, 0)


def reduce_grads(grads, number):
    _, chunks, units, _, lanes = grads.shape
    lats, lons = lax.axis_size("lat"), lax.axis_size("lon")
    side = plane_side(lons)
    sub0 = units // side
    sub1 = sub0 // side
    peers = max(side, lats) - 1
    return pl.pallas_call(
        functools.partial(reduce_kernel, side, lats),
        out_shape=jax.ShapeDtypeStruct(grads.shape, BF16),
        in_specs=[pl.BlockSpec(memory_space=pl.ANY)],
        out_specs=pl.BlockSpec(memory_space=pl.ANY),
        scratch_shapes=[
            pltpu.VMEM((2, chunks, units, 8, lanes), BF16),
            pltpu.VMEM((2, chunks, units, 8, lanes), BF16),
            pltpu.VMEM((chunks, units, 8, lanes), BF16),
            pltpu.VMEM((chunks, units, 8, lanes), BF16),
            pltpu.VMEM((chunks, side - 1, sub0, 8, lanes), BF16),
            pltpu.VMEM((chunks, side - 1, sub1, 8, lanes), BF16),
            pltpu.VMEM((chunks, lats - 1, sub1 // lats, 8, lanes), BF16),
            pltpu.SemaphoreType.DMA((chunks, 8, peers)),
            pltpu.SemaphoreType.DMA((chunks, 8, peers)),
            pltpu.SemaphoreType.DMA((2, 2, chunks)),
        ],
        compiler_params=pltpu.CompilerParams(
            collective_id=number, has_side_effects=True, vmem_limit_bytes=56 * 2**20
        ),
        name="reduce_grads",
    )(grads)


def plane_side(lons):
    return int(round((lons // 2) ** 0.5))


def ring_fits(lats, lons):
    side = plane_side(lons)
    return side >= 2 and lats >= 2 and 2 * side * side == lons and UNITS % (side * side * lats) == 0


def reduce_all(d_w_in_t, d_w_out, d_taps):
    lats, lons = lax.axis_size("lat"), lax.axis_size("lon")
    hidden, channels = d_w_out.shape
    rows = UNITS * 8
    if not ring_fits(lats, lons):
        values = (d_w_in_t.astype(F32), d_w_out.astype(F32), d_taps)
        d_w_in_t, d_w_out, d_taps = lax.psum(values, ("lat", "lon"))
        return d_w_in_t.T, d_w_out, d_taps
    total = pl.cdiv(hidden + d_taps.shape[0], rows) * rows
    low = jnp.pad(d_taps.astype(BF16), ((0, total - hidden - d_taps.shape[0]), (0, 0)))
    first = jnp.concatenate([d_w_out, low], axis=0)
    second = jnp.pad(d_w_in_t, ((0, total - hidden), (0, 0)))
    grads = jnp.stack([first, second]).reshape(2, total // rows, UNITS, 8, channels)
    done = reduce_grads(grads, 2).reshape(2, total, channels)
    return (
        done[1, :hidden].T.astype(F32),
        done[0, :hidden].astype(F32),
        done[0, hidden : hidden + d_taps.shape[0]].astype(F32),
    )


def spread_kernel(ker_ref, taps):
    for t in range(KS * KS):
        taps[t] = jnp.broadcast_to(ker_ref[t : t + 1, :].astype(F32), (8, 128))


def conv_tile(rows_ref, taps, strip, height, flip):
    sums = [None] * height
    for j in range(KS):
        column = [taps[KS * KS - 1 - (i * KS + j) if flip else i * KS + j] for i in range(KS)]
        for r in range(height + KS - 1):
            x = rows_ref[r, pl.ds(strip * 8 + EDGE - HALF + j, 8), :]
            for i in range(KS):
                h = r - i
                if 0 <= h < height:
                    term = column[i] * x
                    sums[h] = term if sums[h] is None else sums[h] + term
    return sums


def forward_kernel(p_ref, ker_ref, o_ref, rows_ref, taps):
    batches, height, width, _ = o_ref.shape
    spread_kernel(ker_ref, taps)

    def batch(m, carry):
        for r in range(height + KS - 1):
            rows_ref[r] = p_ref[m, r].astype(F32)
        for strip in range(width // 8):
            sums = conv_tile(rows_ref, taps, strip, height, False)
            for h in range(height):
                o_ref[m, h, pl.ds(strip * 8, 8), :] = sums[h]
        return carry

    lax.fori_loop(0, batches, batch, 0)


def depthwise(padded, kernel, shape):
    batches, height, width, channels = shape
    tall, wide = height + KS - 1, width + 2 * EDGE
    return pl.pallas_call(
        forward_kernel,
        grid=(pl.cdiv(channels, 128),),
        in_specs=[
            pl.BlockSpec((batches, tall, wide, 128), lambda c: (0, 0, 0, c)),
            pl.BlockSpec((KS * KS, 128), lambda c: (0, c)),
        ],
        out_specs=pl.BlockSpec((batches, height, width, 128), lambda c: (0, 0, 0, c)),
        out_shape=jax.ShapeDtypeStruct(shape, F32),
        scratch_shapes=[pltpu.VMEM((tall, wide, 128), F32), pltpu.VMEM((KS * KS, 8, 128), F32)],
        name="depthwise",
    )(padded, kernel)


def backward_kernel(
    p_ref, d_ref, ker_ref, g_ref, share_ref, o_ref, k_ref, rows_ref, grads_ref, taps, sums_ref
):
    batches, height, width, _ = o_ref.shape
    spread_kernel(ker_ref, taps)
    sums_ref[...] = jnp.zeros_like(sums_ref)

    def batch(m, carry):
        for r in range(height + KS - 1):
            rows_ref[r] = p_ref[m, r].astype(F32)
            grads_ref[r] = d_ref[m, r].astype(F32)
        share = share_ref[m]
        for strip in range(width // 8):
            sums = conv_tile(grads_ref, taps, strip, height, True)
            for h in range(height):
                g = g_ref[m, h, pl.ds(strip * 8, 8), :].astype(F32) * share
                o_ref[m, h, pl.ds(strip * 8, 8), :] = (g + sums[h]).astype(BF16)
            own = [grads_ref[h + HALF, pl.ds(strip * 8 + EDGE, 8), :] for h in range(height)]
            for j in range(KS):
                parts = [sums_ref[i * KS + j] for i in range(KS)]
                for r in range(height + KS - 1):
                    x = rows_ref[r, pl.ds(strip * 8 + EDGE - HALF + j, 8), :]
                    for i in range(KS):
                        h = r - i
                        if 0 <= h < height:
                            parts[i] = parts[i] + own[h] * x
                for i in range(KS):
                    sums_ref[i * KS + j] = parts[i]
        return carry

    lax.fori_loop(0, batches, batch, 0)
    for t in range(KS * KS):
        k_ref[t : t + 1, :] = jnp.sum(sums_ref[t], axis=0, keepdims=True)


def depthwise_back(padded, d_padded, kernel, cotangent, shares):
    batches, height, width, channels = cotangent.shape
    tall, wide = height + KS - 1, width + 2 * EDGE
    tile = pl.BlockSpec((batches, tall, wide, 128), lambda c: (0, 0, 0, c))
    own = pl.BlockSpec((batches, height, width, 128), lambda c: (0, 0, 0, c))
    taps = pl.BlockSpec((KS * KS, 128), lambda c: (0, c))
    return pl.pallas_call(
        backward_kernel,
        grid=(pl.cdiv(channels, 128),),
        in_specs=[tile, tile, taps, own, pl.BlockSpec(memory_space=pltpu.SMEM)],
        out_specs=[own, taps],
        out_shape=[
            jax.ShapeDtypeStruct(cotangent.shape, BF16),
            jax.ShapeDtypeStruct((KS * KS, channels), F32),
        ],
        scratch_shapes=[
            pltpu.VMEM((tall, wide, 128), F32),
            pltpu.VMEM((tall, wide, 128), F32),
            pltpu.VMEM((KS * KS, 8, 128), F32),
            pltpu.VMEM((KS * KS, 8, 128), F32),
        ],
        name="depthwise_back",
    )(padded, d_padded, kernel, cotangent, shares)


def smooth_gate(values):
    return jax.nn.gelu(values, approximate=True)


def body(
    inputs,
    conv_kernel,
    norm_gain,
    norm_shift,
    w_in,
    b_in,
    w_out,
    b_out,
    ocean_mask,
    lengths,
    cotangent,
):
    batches, tile_rows, tile_cols, channels = inputs.shape
    padded = with_halo(inputs)
    taps = conv_kernel.reshape(KS * KS, channels)
    convolved = depthwise(padded, taps, inputs.shape)
    ocean_cells = ocean_mask.astype(F32)[None, :, :, None]
    local_count = jnp.sum(ocean_mask).astype(F32) * batches
    local_mean = jnp.sum(convolved * ocean_cells, axis=(0, 1, 2)) / jnp.maximum(local_count, 1.0)
    off = convolved - local_mean
    local_squares = jnp.sum(off * off * ocean_cells, axis=(0, 1, 2))
    moments = jnp.zeros((8, channels), F32)
    moments = moments.at[0].set(local_mean).at[1].set(local_squares).at[2].set(local_count)
    moments = exchange(merge_moments, moments, 0)
    mean_value, cell_count = moments[0], moments[2, 0]
    inv_std = lax.rsqrt(moments[1] / cell_count + epsilon)
    standard = (convolved - mean_value) * inv_std
    gain_vec = norm_gain.astype(F32)
    normed = (standard * gain_vec + norm_shift.astype(F32)).astype(BF16).reshape(-1, channels)
    pre_gate = jnp.dot(normed, w_in, preferred_element_type=F32) + b_in.astype(F32)
    activated, gate_back = jax.vjp(smooth_gate, pre_gate)
    act_low = activated.astype(BF16)
    branch = jnp.dot(act_low, w_out, preferred_element_type=F32) + b_out.astype(F32)
    output = (inputs.astype(F32) + ocean_cells * branch.reshape(inputs.shape)).astype(BF16)
    kept_steps = lengths.astype(F32) / ROLLOUT
    d_output = cotangent.astype(F32) * kept_steps[:, None, None, None]
    d_branch = (d_output * ocean_cells).reshape(-1, channels)
    branch_low = d_branch.astype(BF16)
    local_b_out = jnp.sum(d_branch, axis=0)
    local_w_out = lax.dot_general(
        act_low, branch_low, (((0,), (0,)), ((), ())), preferred_element_type=F32
    ).astype(BF16)
    d_act = lax.dot_general(branch_low, w_out, (((1,), (1,)), ((), ())), preferred_element_type=F32)
    d_pre = gate_back(d_act)[0]
    pre_low = d_pre.astype(BF16)
    local_b_in = jnp.sum(d_pre, axis=0)
    local_w_in = lax.dot_general(
        pre_low, normed, (((0,), (0,)), ((), ())), preferred_element_type=F32
    ).astype(BF16)
    d_normed = lax.dot_general(
        pre_low, w_in, (((1,), (1,)), ((), ())), preferred_element_type=F32
    ).reshape(inputs.shape)
    sums = jnp.zeros((8, channels), F32)
    sums = sums.at[0].set(jnp.sum(d_normed, axis=(0, 1, 2)))
    sums = sums.at[1].set(jnp.sum(d_normed * standard, axis=(0, 1, 2)))
    sums = sums.at[2].set(local_b_out)
    spread = pl.cdiv(b_in.shape[0], channels)
    sums = sums.at[3 : 3 + spread].set(
        jnp.pad(local_b_in, (0, spread * channels - b_in.shape[0])).reshape(spread, channels)
    )
    sums = exchange(merge_sum, sums, 1)
    d_shift, d_gain, d_b_out = sums[0], sums[1], sums[2]
    d_b_in = sums[3 : 3 + spread].reshape(-1)[: b_in.shape[0]]
    d_conv = (
        gain_vec * inv_std * (d_normed - ocean_cells * (d_shift + standard * d_gain) / cell_count)
    )
    d_padded = with_halo(d_conv.astype(BF16))
    d_inputs, local_kernel = depthwise_back(padded, d_padded, taps, cotangent, kept_steps)
    d_w_in, d_w_out, d_kernel = reduce_all(local_w_in, local_w_out, local_kernel)
    return (
        output,
        d_inputs,
        d_kernel.reshape(conv_kernel.shape),
        d_gain,
        d_shift,
        d_w_in,
        d_b_in,
        d_w_out,
        d_b_out,
    )


def solution(mesh):
    tile = P(None, "lat", "lon", None)
    in_specs = (tile, P(), P(), P(), P(), P(), P(), P(), P("lat", "lon"), P(), tile)
    out_specs = (tile, tile, P(), P(), P(), P(), P(), P(), P())
    return jax.shard_map(body, mesh=mesh, in_specs=in_specs, out_specs=out_specs, check_vma=False)
```
